8 devices in a mesh: row: 2 (over z, y), col: 4 (over x, core).
Axes of the slice: x: 2, y: 2, z: 1, core: 2. Of those that a mesh axis runs over, the one named last changes fastest.
Arguments:
- v_panels: float32 [8192, 8192], P('row', 'col')
- t_factors: float32 [128, 64, 64], P('col')
- z_vecs: float32 [8192, 2048], P(None, ('row', 'col'))
Outputs:
- output: float32 [8192, 2048], P(None, ('row', 'col'))
All inputs are finite; a program needn't handle non-finite values.
Results may differ from the reference program's by a relative error of at most 0.001.
Values sent between devices are 32-bit elements.
A program may use at most 1 GiB of HBM per device.

```python
import jax
import jax.numpy as jnp
from jax import lax

N = 8192
BLOCK = 64
K_DEV = 256
ROW_DEV = 2
COL_DEV = 4

NPANEL = N // BLOCK
M_LOC = NPANEL // COL_DEV
K_COLS = K_DEV * ROW_DEV * COL_DEV


def build_inputs(raw_vals, z_vecs):
    row_nat = jnp.arange(N)[:, None, None]
    diag_row = (jnp.arange(NPANEL) * BLOCK)[None, :, None] + jnp.arange(BLOCK)[None, None, :]
    v_nat = jnp.where(row_nat > diag_row, raw_vals, jnp.where(row_nat == diag_row, 1.0, 0.0)).astype(raw_vals.dtype)
    gram = jnp.einsum("nmb,nmc->mbc", v_nat, v_nat, precision=lax.Precision.HIGHEST)
    half_diag = 0.5 * jnp.diagonal(gram, axis1=1, axis2=2)
    t_inverse = jnp.triu(gram, 1) + jnp.eye(BLOCK, dtype=raw_vals.dtype) * half_diag[:, None, :]
    t_nat = jnp.triu(jnp.linalg.inv(t_inverse))
    v_cols = v_nat.reshape(N, M_LOC, COL_DEV, BLOCK).transpose(0, 2, 1, 3).reshape(N, N)
    v_store = v_cols.reshape(NPANEL // ROW_DEV, ROW_DEV, BLOCK, N).transpose(1, 0, 2, 3).reshape(N, N)
    t_store = t_nat.reshape(M_LOC, COL_DEV, BLOCK, BLOCK).transpose(1, 0, 2, 3).reshape(NPANEL, BLOCK, BLOCK)
    return {"v_panels": v_store, "t_factors": t_store, "z_vecs": z_vecs}


def setup_inputs(seed: int = 0) -> dict:
    base_key = jax.random.key(seed)
    key_v, key_z = jax.random.split(base_key)
    raw_vals = jax.random.normal(key_v, (N, NPANEL, BLOCK), jnp.float32)
    z_vecs = jax.random.normal(key_z, (N, K_COLS), jnp.float32)
    return build_inputs(raw_vals, z_vecs)


def reference(v_panels, t_factors, z_vecs):
    def apply_panel(x_cur, panel_idx):
        store_slot = (panel_idx % COL_DEV) * M_LOC + panel_idx // COL_DEV
        v_blk = lax.dynamic_slice_in_dim(v_panels, store_slot * BLOCK, BLOCK, axis=1)
        t_blk = lax.dynamic_index_in_dim(t_factors, store_slot, axis=0, keepdims=False)
        w_blk = jnp.dot(v_blk.T, x_cur, precision=lax.Precision.HIGHEST, preferred_element_type=jnp.float32)
        y_blk = jnp.dot(t_blk, w_blk, precision=lax.Precision.HIGHEST, preferred_element_type=jnp.float32)
        x_new = x_cur - jnp.dot(v_blk, y_blk, precision=lax.Precision.HIGHEST, preferred_element_type=jnp.float32)
        return x_new, None

    x_out, _ = lax.scan(apply_panel, z_vecs, jnp.arange(NPANEL - 1, -1, -1))
    return x_out
```

```python
import functools

import jax
import jax.numpy as jnp
from jax import lax
from jax.experimental import pallas as pl
from jax.experimental.pallas import tpu as pltpu
from jax.sharding import PartitionSpec as P

HI = lax.Precision.HIGHEST
F32 = jnp.float32
BF16 = jnp.bfloat16
MESH_ID = pl.DeviceIdType.MESH
NN = (((1,), (0,)), ((), ()))
NT = (((1,), (1,)), ((), ()))

LANES = 128
STRIP = 256


def split3(a):
    a1 = a.astype(BF16)
    rest = a - a1.astype(F32)
    a2 = rest.astype(BF16)
    a3 = (rest - a2.astype(F32)).astype(BF16)
    return a1, a2, a3


def dot6(a, b, dims):
    a1, a2, a3 = a
    b1, b2, b3 = b

    def one(p, q):
        return lax.dot_general(p, q, dims, preferred_element_type=F32)

    return ((((one(a3, b1) + one(a1, b3)) + one(a2, b2)) + one(a2, b1)) + one(a1, b2)) + one(a1, b1)


def exact(a, b, dims):
    return lax.dot_general(a, b, dims, precision=HI, preferred_element_type=F32)


def kernel(blocks, v_ref, t_ref, z_ref, x_out, vg, x_ref, tg, vbuf, v1s, v2s, v3s, wt, gram, gram_q,
           send_sem, recv_sem, tsend_sem, trecv_sem, load_sem, z_sem):
    y = lax.axis_index("row")
    col = lax.axis_index("col")
    xx = col // 2
    core = lax.rem(col, 2)
    q_own = col
    q_x = (1 - xx) * 2 + core
    q_c = xx * 2 + (1 - core)
    q_xc = (1 - xx) * 2 + (1 - core)
    dev_x = (y, q_x)
    dev_y = (1 - y, q_own)
    dev_c = (y, q_c)
    dev_xc = (y, q_xc)
    half_rows = blocks * STRIP

    def rcopy(s, kind, src, dst, dev):
        return lambda: pltpu.make_async_remote_copy(
            src_ref=src, dst_ref=dst, send_sem=send_sem.at[s, kind], recv_sem=recv_sem.at[s, kind],
            device_id=dev, device_id_type=MESH_ID)

    def rows(s):
        return pl.ds(s * STRIP, half_rows - s * STRIP)

    def halves(s):
        n = half_rows - s * STRIP
        return pl.ds(s * STRIP, n // 2), pl.ds(s * STRIP + n // 2, n // 2)

    def own(s):
        return v_ref.at[rows(s), pl.ds(s * LANES, LANES)]

    def stage_a(s):
        dst = vg.at[s, y, q_own, rows(s)]
        return [rcopy(s, 0, own(s), dst, dev_x), rcopy(s, 1, own(s), dst, dev_y), rcopy(s, 2, own(s), dst, dev_c)]

    def stage_t(s):
        def tcopy(k, dev):
            return lambda: pltpu.make_async_remote_copy(
                src_ref=t_ref.at[s], dst_ref=tg.at[s, q_own], send_sem=tsend_sem.at[s, k], recv_sem=trecv_sem.at[s, k],
                device_id=dev, device_id_type=MESH_ID)

        return [tcopy(k, dev) for k, dev in enumerate((dev_x, dev_c, dev_xc))]

    def stage_f(s):
        first, second = halves(s)
        from_x = vg.at[s, y, q_x]
        from_y = vg.at[s, 1 - y, q_own]
        return [rcopy(s, 3, from_x.at[first], from_x.at[first], dev_y),
                rcopy(s, 4, from_y.at[second], from_y.at[second], dev_x),
                rcopy(s, 5, from_x.at[rows(s)], from_x.at[rows(s)], dev_c),
                rcopy(s, 6, from_y.at[rows(s)], from_y.at[rows(s)], dev_c)]

    def stage_g(s):
        first, second = halves(s)
        diag = vg.at[s, 1 - y, q_x]
        return [rcopy(s, 7, diag.at[first], diag.at[first], dev_c),
                rcopy(s, 8, diag.at[second], diag.at[second], dev_c)]

    def start_a(s):
        for c in stage_a(s) + stage_t(s):
            c().start()

    def start_f(s):
        a = stage_a(s)
        a[0]().wait_recv()
        a[1]().wait_recv()
        for c in stage_f(s):
            c().start()

    def start_g(s):
        f = stage_f(s)
        f[0]().wait_recv()
        f[1]().wait_recv()
        for c in stage_g(s):
            c().start()

    def finish(s):
        a, f, g, t = stage_a(s), stage_f(s), stage_g(s), stage_t(s)
        for c in (a[2], f[2], f[3], g[0], g[1], *t):
            c().wait_recv()
        for c in (*a, *f, *g, *t):
            c().wait_send()

    z_copy = pltpu.make_async_copy(z_ref, x_ref, z_sem.at[0])
    z_copy.start()
    t_copy = pltpu.make_async_copy(t_ref, tg.at[:, q_own], z_sem.at[1])
    t_copy.start()
    start_a(blocks - 1)
    start_a(blocks - 2)
    start_f(blocks - 1)
    t_copy.wait()
    z_copy.wait()

    lane = lax.broadcasted_iota(jnp.int32, (64, LANES), 1)
    row_h = (lax.broadcasted_iota(jnp.int32, (LANES, LANES), 0) // 64) % 2
    col_h = (lax.broadcasted_iota(jnp.int32, (LANES, LANES), 1) // 64) % 2
    same_half = jnp.where(row_h == col_h, 1.0, 0.0).astype(F32)
    next_half = jnp.where(row_h < col_h, 1.0, 0.0).astype(F32)

    def block_step(i, carry):
        for k in range(blocks):
            @pl.when(i == k)
            def _():
                s = blocks - 1 - k
                if s >= 2:
                    start_a(s - 2)
                if s >= 1:
                    start_f(s - 1)
                start_g(s)
                finish(s)

        s = blocks - 1 - i
        n = i + 1
        total = 2 * n

        def place(t):
            dy = jnp.where(t >= n, 1, 0)
            rr = t - dy * n
            yy = jnp.where(dy == 0, y, 1 - y)
            row0 = pl.multiple_of((s + rr) * STRIP, STRIP)
            return dy, yy, row0

        def load(t, slot):
            dy, yy, row0 = place(t)
            r = pl.ds(row0, STRIP)

            def put(src, q, k):
                return pltpu.make_async_copy(
                    src, vbuf.at[slot, :, pl.ds(pl.multiple_of(q * LANES, LANES), LANES)], load_sem.at[slot, k])

            @pl.when(dy == 0)
            def _():
                put(v_ref.at[r, pl.ds(pl.multiple_of(s * LANES, LANES), LANES)], q_own, 0).start()

            @pl.when(dy != 0)
            def _():
                put(vg.at[s, yy, q_own, r], q_own, 0).start()

            for k, q in ((1, q_x), (2, q_c), (3, q_xc)):
                put(vg.at[s, yy, q, r], q, k).start()

        def load_wait(slot):
            for k, q in ((0, q_own), (1, q_x), (2, q_c), (3, q_xc)):
                pltpu.make_async_copy(
                    vg.at[0, 0, 0, pl.ds(0, STRIP)],
                    vbuf.at[slot, :, pl.ds(pl.multiple_of(q * LANES, LANES), LANES)], load_sem.at[slot, k]).wait()

        wt[...] = jnp.zeros_like(wt)
        gram[...] = jnp.zeros_like(gram)
        gram_q[...] = jnp.zeros_like(gram_q)
        load(0, 0)

        def pass_one(t, c):
            slot = lax.rem(t, 2)

            @pl.when(t + 1 < total)
            def _():
                load(t + 1, 1 - slot)

            load_wait(slot)
            _, yy, row0 = place(t)
            v1, v2, v3 = split3(vbuf[slot])
            keep = pl.ds(pl.multiple_of(t * STRIP, STRIP), STRIP)
            v1s[keep, :] = v1
            v2s[keep, :] = v2
            v3s[keep, :] = v3
            xs = split3(x_ref[:, pl.ds(pl.multiple_of(yy * half_rows + row0, STRIP), STRIP)])
            wt[...] += dot6(xs, (v1, v2, v3), NN)
            v1t = v1.T
            v2t = v2.T
            one = functools.partial(lax.dot_general, dimension_numbers=NN, preferred_element_type=F32)
            gram[...] += one(v2t, v2) + one(v1t, v1)
            gram_q[...] += one(v1t, v3) + one(v1t, v2)
            return c

        lax.fori_loop(0, total, pass_one, 0)

        gq = gram_q[...]
        g = gram[...] + (gq + gq.T)

        tq = []
        for q in range(4):
            tt = tg[s, q]
            tq.append(jnp.concatenate([jnp.where(lane < 64, tt, 0.0), jnp.where(lane >= 64, tt, 0.0)], axis=0))

        def gq_blk(a, b):
            return g[a * LANES:(a + 1) * LANES, b * LANES:(b + 1) * LANES]

        def merge(ta, gab, tb):
            return -exact(exact(ta, gab, NN), tb, NN)

        zero = jnp.zeros((LANES, LANES), F32)
        t01 = merge(tq[0], gq_blk(0, 1) * same_half, tq[1])
        t23 = merge(tq[2], gq_blk(2, 3) * same_half, tq[3])
        ta = jnp.concatenate([jnp.concatenate([tq[0], t01], axis=1), jnp.concatenate([zero, tq[1]], axis=1)], axis=0)
        tb = jnp.concatenate([jnp.concatenate([tq[2], t23], axis=1), jnp.concatenate([zero, tq[3]], axis=1)], axis=0)
        gab = jnp.concatenate([jnp.concatenate([gq_blk(a, b) * same_half for b in (2, 3)], axis=1) for a in (0, 1)], axis=0)
        tab = merge(ta, gab, tb)
        zero2 = jnp.zeros((2 * LANES, 2 * LANES), F32)
        tfull = jnp.concatenate([jnp.concatenate([ta, tab], axis=1), jnp.concatenate([zero2, tb], axis=1)], axis=0)
        g3 = jnp.concatenate([jnp.concatenate([gq_blk(a, b) * next_half for b in range(4)], axis=1) for a in range(4)], axis=0)

        y1t = exact(wt[...], tfull, NT)
        yt = y1t - exact(exact(y1t, g3, NT), tfull, NT)
        ys = split3(yt)

        def pass_two(t, c):
            _, yy, row0 = place(t)
            keep = pl.ds(pl.multiple_of(t * STRIP, STRIP), STRIP)
            vs = (v1s[keep, :], v2s[keep, :], v3s[keep, :])
            cols = pl.ds(pl.multiple_of(yy * half_rows + row0, STRIP), STRIP)
            x_ref[:, cols] = x_ref[:, cols] - dot6(ys, vs, NT)
            return c

        lax.fori_loop(0, total, pass_two, 0)
        return carry

    lax.fori_loop(0, blocks, block_step, 0)
    out = pltpu.make_async_copy(x_ref, x_out, z_sem.at[0])
    out.start()
    out.wait()


def solution(mesh):
    def local_apply(v_loc, t_loc, z_loc):
        n, k = z_loc.shape
        blocks = v_loc.shape[1] // LANES
        half_rows = v_loc.shape[0]
        wide = 4 * LANES
        t_pack = t_loc.reshape(blocks, 2, 64, 64).transpose(0, 2, 1, 3).reshape(blocks, 64, LANES)
        z_t = z_loc.T
        hbm = pl.BlockSpec(memory_space=pl.ANY)
        x_t, _ = pl.pallas_call(
            functools.partial(kernel, blocks),
            out_shape=(jax.ShapeDtypeStruct((k, n), F32),
                       jax.ShapeDtypeStruct((blocks, 2, 4, half_rows, LANES), F32)),
            in_specs=[hbm, pl.BlockSpec(memory_space=pltpu.VMEM), hbm],
            out_specs=(hbm, hbm),
            scratch_shapes=[
                pltpu.VMEM((k, n), F32),
                pltpu.VMEM((blocks, 4, 64, LANES), F32),
                pltpu.VMEM((2, STRIP, wide), F32),
                pltpu.VMEM((n, wide), BF16),
                pltpu.VMEM((n, wide), BF16),
                pltpu.VMEM((n, wide), BF16),
                pltpu.VMEM((k, wide), F32),
                pltpu.VMEM((wide, wide), F32),
                pltpu.VMEM((wide, wide), F32),
                pltpu.SemaphoreType.DMA((blocks, 9)),
                pltpu.SemaphoreType.DMA((blocks, 9)),
                pltpu.SemaphoreType.DMA((blocks, 3)),
                pltpu.SemaphoreType.DMA((blocks, 3)),
                pltpu.SemaphoreType.DMA((2, 4)),
                pltpu.SemaphoreType.DMA((2,)),
            ],
            compiler_params=pltpu.CompilerParams(has_side_effects=True, vmem_limit_bytes=64000 * 1024),
        )(v_loc, t_pack, z_t)
        return x_t.T

    return jax.shard_map(
        local_apply,
        mesh=mesh,
        in_specs=(P("row", "col"), P("col", None, None), P(None, ("row", "col"))),
        out_specs=P(None, ("row", "col")),
        check_vma=False,
    )
```

```python
import functools

import jax
import jax.numpy as jnp
from jax import lax
from jax.experimental import pallas as pl
from jax.experimental.pallas import tpu as pltpu
from jax.sharding import PartitionSpec as P

HI = lax.Precision.HIGHEST
F32 = jnp.float32
BF16 = jnp.bfloat16
MESH_ID = pl.DeviceIdType.MESH
NN = (((1,), (0,)), ((), ()))
NT = (((1,), (1,)), ((), ()))

LANES = 128
STRIP = 256


def split3(a):
    a1 = a.astype(BF16)
    rest = a - a1.astype(F32)
    a2 = rest.astype(BF16)
    a3 = (rest - a2.astype(F32)).astype(BF16)
    return a1, a2, a3


def dot6(a, b, dims):
    a1, a2, a3 = a
    b1, b2, b3 = b

    def one(p, q):
        return lax.dot_general(p, q, dims, preferred_element_type=F32)

    return ((((one(a3, b1) + one(a1, b3)) + one(a2, b2)) + one(a2, b1)) + one(a1, b2)) + one(a1, b1)


def exact(a, b, dims):
    return lax.dot_general(a, b, dims, precision=HI, preferred_element_type=F32)


def kernel(blocks, v_ref, t_ref, z_ref, x_out, vg, x_ref, z_buf, tg, vbuf, v1s, v2s, v3s, wt, gram, gram_q, g_in,
           send_sem, recv_sem, tsend_sem, trecv_sem, gsend_sem, grecv_sem, load_sem, z_sem):
    y = lax.axis_index("row")
    col = lax.axis_index("col")
    xx = col // 2
    core = lax.rem(col, 2)
    q_own = col
    q_x = (1 - xx) * 2 + core
    q_c = xx * 2 + (1 - core)
    q_xc = (1 - xx) * 2 + (1 - core)
    dev_x = (y, q_x)
    dev_y = (1 - y, q_own)
    dev_c = (y, q_c)
    dev_xc = (y, q_xc)
    half_rows = blocks * STRIP
    units = 2 * blocks

    def span(u):
        i, h = u // 2, u % 2
        n = i + 1
        first = (n + 1) // 2
        begin, size = (0, first) if h == 0 else (first, n - first)
        return blocks - 1 - i, (blocks - 1 - i + begin) * STRIP, size * STRIP

    def live(u):
        return 0 <= u < units and span(u)[2] > 0

    def rcopy(u, kind, src, dst, dev):
        return lambda: pltpu.make_async_remote_copy(
            src_ref=src, dst_ref=dst, send_sem=send_sem.at[u, kind], recv_sem=recv_sem.at[u, kind],
            device_id=dev, device_id_type=MESH_ID)

    def stage_a(u):
        s, begin, size = span(u)
        r = pl.ds(begin, size)
        src = v_ref.at[r, pl.ds(s * LANES, LANES)]
        dst = vg.at[s, y, q_own, r]
        return [rcopy(u, 0, src, dst, dev_x), rcopy(u, 1, src, dst, dev_y), rcopy(u, 2, src, dst, dev_c)]

    def stage_t(s):
        def tcopy(k, dev):
            return lambda: pltpu.make_async_remote_copy(
                src_ref=t_ref.at[s], dst_ref=tg.at[s, q_own], send_sem=tsend_sem.at[s, k], recv_sem=trecv_sem.at[s, k],
                device_id=dev, device_id_type=MESH_ID)

        return [tcopy(k, dev) for k, dev in enumerate((dev_x, dev_c, dev_xc))]

    def stage_f(u):
        s, begin, size = span(u)
        first, second, r = pl.ds(begin, size // 2), pl.ds(begin + size // 2, size // 2), pl.ds(begin, size)
        from_x = vg.at[s, y, q_x]
        from_y = vg.at[s, 1 - y, q_own]
        return [rcopy(u, 3, from_x.at[first], from_x.at[first], dev_y),
                rcopy(u, 4, from_y.at[second], from_y.at[second], dev_x),
                rcopy(u, 5, from_x.at[r], from_x.at[r], dev_c),
                rcopy(u, 6, from_y.at[r], from_y.at[r], dev_c)]

    def stage_g(u):
        s, begin, size = span(u)
        first, second = pl.ds(begin, size // 2), pl.ds(begin + size // 2, size // 2)
        diag = vg.at[s, 1 - y, q_x]
        return [rcopy(u, 7, diag.at[first], diag.at[first], dev_c),
                rcopy(u, 8, diag.at[second], diag.at[second], dev_c)]

    def start_a(u):
        if live(u):
            if u % 2 == 0:
                for c in stage_t(span(u)[0]):
                    c().start()
            for c in stage_a(u):
                c().start()

    def start_f(u):
        if live(u):
            a = stage_a(u)
            a[0]().wait_recv()
            a[1]().wait_recv()
            for c in stage_f(u):
                c().start()

    def start_g(u):
        if live(u):
            a, f = stage_a(u), stage_f(u)
            f[0]().wait_recv()
            f[1]().wait_recv()
            g = stage_g(u)
            for c in g:
                c().start()
            if u % 2 == 0:
                for c in stage_t(span(u)[0]):
                    c().wait_recv()
            for c in (a[2], f[2], f[3], g[0], g[1]):
                c().wait_recv()

    def drain(u):
        if live(u):
            if u % 2 == 0:
                for c in stage_t(span(u)[0]):
                    c().wait_send()
            for c in (*stage_a(u), *stage_f(u), *stage_g(u)):
                c().wait_send()

    start_a(0)
    start_a(2)
    start_a(3)
    t_copy = pltpu.make_async_copy(t_ref, tg.at[:, q_own], z_sem.at[1])
    t_copy.start()
    z_copy = pltpu.make_async_copy(z_ref, z_buf, z_sem.at[0])
    z_copy.start()
    start_f(0)
    t_copy.wait()
    z_copy.wait()

    lane = lax.broadcasted_iota(jnp.int32, (64, LANES), 1)
    row_h = (lax.broadcasted_iota(jnp.int32, (LANES, LANES), 0) // 64) % 2
    col_h = (lax.broadcasted_iota(jnp.int32, (LANES, LANES), 1) // 64) % 2
    same_half = jnp.where(row_h == col_h, 1.0, 0.0).astype(F32)
    next_half = jnp.where(row_h < col_h, 1.0, 0.0).astype(F32)
    one = functools.partial(lax.dot_general, dimension_numbers=NN, preferred_element_type=F32)

    def block_step(i, carry):
        s = blocks - 1 - i
        n = i + 1
        n_first = (n + 1) // 2

        def row_of(t):
            return pl.multiple_of((s + t) * STRIP, STRIP)

        def x_cols(t):
            r = row_of(t)
            return (pl.ds(pl.multiple_of(y * half_rows + r, STRIP), STRIP),
                    pl.ds(pl.multiple_of((1 - y) * half_rows + r, STRIP), STRIP))

        def keep(t):
            return pl.ds(pl.multiple_of(t * 2 * STRIP, 2 * STRIP), 2 * STRIP)

        def put(src, slot, dy, q, k):
            return pltpu.make_async_copy(
                src, vbuf.at[slot, pl.ds(dy * STRIP, STRIP), pl.ds(pl.multiple_of(q * LANES, LANES), LANES)],
                load_sem.at[slot, dy, k])

        def load(t, slot):
            r = pl.ds(row_of(t), STRIP)
            put(v_ref.at[r, pl.ds(pl.multiple_of(s * LANES, LANES), LANES)], slot, 0, q_own, 0).start()
            for k, q in ((1, q_x), (2, q_c), (3, q_xc)):
                put(vg.at[s, y, q, r], slot, 0, q, k).start()
            for k, q in ((0, q_own), (1, q_x), (2, q_c), (3, q_xc)):
                put(vg.at[s, 1 - y, q, r], slot, 1, q, k).start()

        def load_wait(slot):
            for dy in (0, 1):
                for k, q in ((0, q_own), (1, q_x), (2, q_c), (3, q_xc)):
                    put(vg.at[0, 0, 0, pl.ds(0, STRIP)], slot, dy, q, k).wait()

        def take_in(lo, hi):
            @pl.when(lo < hi)
            def _():
                load(lo, lax.rem(lo, 2))

            def body(t, c):
                slot = lax.rem(t, 2)

                @pl.when(t + 1 < hi)
                def _():
                    load(t + 1, 1 - slot)

                load_wait(slot)
                v1, v2, v3 = split3(vbuf[slot])
                v1s[keep(t), :] = v1
                v2s[keep(t), :] = v2
                v3s[keep(t), :] = v3
                mine = pl.ds(pl.multiple_of((t * 2 + core) * STRIP, STRIP), STRIP)
                v1, v2, v3 = v1s[mine, :], v2s[mine, :], v3s[mine, :]
                v1t = v1.T
                v2t = v2.T
                gram[...] += one(v2t, v2) + one(v1t, v1)
                gram_q[...] += one(v1t, v3) + one(v1t, v2)
                return c

            lax.fori_loop(lo, hi, body, 0)

        def project(lo, hi):
            def body(t, c):
                own, other = x_cols(t)
                xs = split3(jnp.concatenate([x_ref[:, own], x_ref[:, other]], axis=1))
                wt[...] += dot6(xs, (v1s[keep(t), :], v2s[keep(t), :], v3s[keep(t), :]), NN)
                return c

            lax.fori_loop(lo, hi, body, 0)

        wt[...] = jnp.zeros_like(wt)
        gram[...] = jnp.zeros_like(gram)
        gram_q[...] = jnp.zeros_like(gram_q)
        own, other = x_cols(0)
        x_ref[:, own] = z_buf[own, :].T
        x_ref[:, other] = z_buf[other, :].T

        for k in range(blocks):
            @pl.when(i == k)
            def _():
                start_g(2 * k)

        take_in(0, n_first)
        project(0, n_first)

        for k in range(blocks):
            @pl.when(i == k)
            def _():
                start_g(2 * k + 1)
                start_f(2 * k + 2)
                start_a(2 * k + 4)

        take_in(n_first, n)
        gq = gram_q[...]
        gram[...] += gq + gq.T
        slot = lax.rem(i, 2)
        g_copy = pltpu.make_async_remote_copy(
            src_ref=gram, dst_ref=g_in.at[slot], send_sem=gsend_sem.at[slot], recv_sem=grecv_sem.at[slot],
            device_id=dev_c, device_id_type=MESH_ID)
        g_copy.start()
        project(n_first, n)
        g_copy.wait()
        g = gram[...] + g_in[slot]

        tq = []
        for q in range(4):
            tt = tg[s, q]
            tq.append(jnp.concatenate([jnp.where(lane < 64, tt, 0.0), jnp.where(lane >= 64, tt, 0.0)], axis=0))

        def gq_blk(a, b):
            return g[a * LANES:(a + 1) * LANES, b * LANES:(b + 1) * LANES]

        def merge(ta, gab, tb):
            return -exact(exact(ta, gab, NN), tb, NN)

        zero = jnp.zeros((LANES, LANES), F32)
        t01 = merge(tq[0], gq_blk(0, 1) * same_half, tq[1])
        t23 = merge(tq[2], gq_blk(2, 3) * same_half, tq[3])
        ta = jnp.concatenate([jnp.concatenate([tq[0], t01], axis=1), jnp.concatenate([zero, tq[1]], axis=1)], axis=0)
        tb = jnp.concatenate([jnp.concatenate([tq[2], t23], axis=1), jnp.concatenate([zero, tq[3]], axis=1)], axis=0)
        gab = jnp.concatenate([jnp.concatenate([gq_blk(a, b) * same_half for b in (2, 3)], axis=1) for a in (0, 1)], axis=0)
        tab = merge(ta, gab, tb)
        zero2 = jnp.zeros((2 * LANES, 2 * LANES), F32)
        tfull = jnp.concatenate([jnp.concatenate([ta, tab], axis=1), jnp.concatenate([zero2, tb], axis=1)], axis=0)
        g3 = jnp.concatenate([jnp.concatenate([gq_blk(a, b) * next_half for b in range(4)], axis=1) for a in range(4)], axis=0)

        y1t = exact(wt[...], tfull, NT)
        yt = y1t - exact(exact(y1t, g3, NT), tfull, NT)
        ys = split3(yt)

        for k in range(blocks):
            @pl.when(i == k)
            def _():
                start_f(2 * k + 3)
                start_a(2 * k + 5)

        def pass_two(t, c):
            own, other = x_cols(t)
            u = dot6(ys, (v1s[keep(t), :], v2s[keep(t), :], v3s[keep(t), :]), NT)
            x_ref[:, own] = x_ref[:, own] - u[:, :STRIP]
            x_ref[:, other] = x_ref[:, other] - u[:, STRIP:]
            return c

        lax.fori_loop(0, n, pass_two, 0)
        return carry

    lax.fori_loop(0, blocks, block_step, 0)
    out = pltpu.make_async_copy(x_ref, x_out, z_sem.at[0])
    out.start()
    for u in range(units):
        drain(u)
    out.wait()


def solution(mesh):
    def local_apply(v_loc, t_loc, z_loc):
        n, k = z_loc.shape
        blocks = v_loc.shape[1] // LANES
        half_rows = v_loc.shape[0]
        wide = 4 * LANES
        t_pack = t_loc.reshape(blocks, 2, 64, 64).transpose(0, 2, 1, 3).reshape(blocks, 64, LANES)
        hbm = pl.BlockSpec(memory_space=pl.ANY)
        x_t, _ = pl.pallas_call(
            functools.partial(kernel, blocks),
            out_shape=(jax.ShapeDtypeStruct((k, n), F32),
                       jax.ShapeDtypeStruct((blocks, 2, 4, half_rows, LANES), F32)),
            in_specs=[hbm, pl.BlockSpec(memory_space=pltpu.VMEM), hbm],
            out_specs=(hbm, hbm),
            scratch_shapes=[
                pltpu.VMEM((k, n), F32),
                pltpu.VMEM((n, k), F32),
                pltpu.VMEM((blocks, 4, 64, LANES), F32),
                pltpu.VMEM((2, 2 * STRIP, wide), F32),
                pltpu.VMEM((n, wide), BF16),
                pltpu.VMEM((n, wide), BF16),
                pltpu.VMEM((n, wide), BF16),
                pltpu.VMEM((k, wide), F32),
                pltpu.VMEM((wide, wide), F32),
                pltpu.VMEM((wide, wide), F32),
                pltpu.VMEM((2, wide, wide), F32),
                pltpu.SemaphoreType.DMA((2 * blocks, 9)),
                pltpu.SemaphoreType.DMA((2 * blocks, 9)),
                pltpu.SemaphoreType.DMA((blocks, 3)),
                pltpu.SemaphoreType.DMA((blocks, 3)),
                pltpu.SemaphoreType.DMA((2,)),
                pltpu.SemaphoreType.DMA((2,)),
                pltpu.SemaphoreType.DMA((2, 2, 4)),
                pltpu.SemaphoreType.DMA((2,)),
            ],
            compiler_params=pltpu.CompilerParams(has_side_effects=True, vmem_limit_bytes=64000 * 1024),
        )(v_loc, t_pack, z_loc)
        return x_t.T

    return jax.shard_map(
        local_apply,
        mesh=mesh,
        in_specs=(P("row", "col"), P("col", None, None), P(None, ("row", "col"))),
        out_specs=P(None, ("row", "col")),
        check_vma=False,
    )
```

```python
import functools

import jax
import jax.numpy as jnp
from jax import lax
from jax.experimental import pallas as pl
from jax.experimental.pallas import tpu as pltpu
from jax.sharding import PartitionSpec as P

HI = lax.Precision.HIGHEST
F32 = jnp.float32
BF16 = jnp.bfloat16
MESH_ID = pl.DeviceIdType.MESH
NN = (((1,), (0,)), ((), ()))
NT = (((1,), (1,)), ((), ()))

LANES = 128
STRIP = 256
AHEAD = 0


def split3(a):
    a1 = a.astype(BF16)
    rest = a - a1.astype(F32)
    a2 = rest.astype(BF16)
    a3 = (rest - a2.astype(F32)).astype(BF16)
    return a1, a2, a3


def dot6(a, b, dims):
    (a1, a2, a3), (b1, b2, b3) = a, b
    (over_a,), (over_b,) = dims[0]
    lhs = jnp.concatenate([a3, a1, a2, a2, a1, a1], axis=over_a)
    rhs = jnp.concatenate([b1, b3, b2, b1, b2, b1], axis=over_b)
    return lax.dot_general(lhs, rhs, dims, preferred_element_type=F32)


def exact(a, b, dims):
    return lax.dot_general(a, b, dims, precision=HI, preferred_element_type=F32)


def kernel(blocks, v_ref, t_ref, z_ref, x_out, vg, x_ref, tg, vbuf, v1s, v2s, v3s, wt, gram, gram_q, g_in,
           send_sem, recv_sem, tsend_sem, trecv_sem, gsend_sem, grecv_sem, load_sem, z_sem):
    y = lax.axis_index("row")
    col = lax.axis_index("col")
    xx = col // 2
    core = lax.rem(col, 2)
    q_own = col
    q_x = (1 - xx) * 2 + core
    q_c = xx * 2 + (1 - core)
    q_xc = (1 - xx) * 2 + (1 - core)
    dev_x = (y, q_x)
    dev_y = (1 - y, q_own)
    dev_c = (y, q_c)
    half_rows = blocks * STRIP
    units = 2 * blocks

    def span(u):
        i, h = u // 2, u % 2
        n = i + 1
        first = (n + 1) // 2
        begin, size = (0, first) if h == 0 else (first, n - first)
        return blocks - 1 - i, (blocks - 1 - i + begin) * STRIP, size * STRIP

    def live(u):
        return 0 <= u < units and span(u)[2] > 0

    def relay_parts(u):
        _, begin, size = span(u)
        cut = size // 2 + (32 if u % 2 == 0 else 0)
        return pl.ds(begin, cut), pl.ds(begin + cut, size - cut)

    order = [u for u in range(units) if span(u)[2] > 0]

    def ahead(p):
        w, strips = p + 1, 0
        while w < len(order) and (w < p + 3 or strips < AHEAD):
            strips += span(order[w])[2] // STRIP
            w += 1
        return w

    def rcopy(u, kind, src, dst, dev):
        return lambda: pltpu.make_async_remote_copy(
            src_ref=src, dst_ref=dst, send_sem=send_sem.at[u, kind], recv_sem=recv_sem.at[u, kind],
            device_id=dev, device_id_type=MESH_ID)

    def stage_a(u):
        s, begin, size = span(u)
        r = pl.ds(begin, size)
        src = v_ref.at[r, pl.ds(s * LANES, LANES)]
        dst = vg.at[s, y, q_own, r]
        return [rcopy(u, 0, src, dst, dev_x), rcopy(u, 1, src, dst, dev_y), rcopy(u, 2, src, dst, dev_c)]

    def stage_t(s):
        def tcopy(k, src, q, dev):
            return lambda: pltpu.make_async_remote_copy(
                src_ref=src, dst_ref=tg.at[s, q], send_sem=tsend_sem.at[s, k], recv_sem=trecv_sem.at[s, k],
                device_id=dev, device_id_type=MESH_ID)

        return [tcopy(0, t_ref.at[s], q_own, dev_x), tcopy(1, t_ref.at[s], q_own, dev_c),
                tcopy(2, tg.at[s, q_x], q_x, dev_c)]

    def stage_f(u):
        s, begin, size = span(u)
        first, second = relay_parts(u)
        r = pl.ds(begin, size)
        from_x = vg.at[s, y, q_x]
        from_y = vg.at[s, 1 - y, q_own]
        return [rcopy(u, 3, from_x.at[first], from_x.at[first], dev_y),
                rcopy(u, 4, from_y.at[second], from_y.at[second], dev_x),
                rcopy(u, 5, from_x.at[r], from_x.at[r], dev_c),
                rcopy(u, 6, from_y.at[r], from_y.at[r], dev_c)]

    def stage_g(u):
        s = span(u)[0]
        first, second = relay_parts(u)
        diag = vg.at[s, 1 - y, q_x]
        return [rcopy(u, 7, diag.at[first], diag.at[first], dev_c),
                rcopy(u, 8, diag.at[second], diag.at[second], dev_c)]

    def start_a(u):
        if live(u):
            if u % 2 == 0:
                for c in stage_t(span(u)[0])[:2]:
                    c().start()
            for c in stage_a(u):
                c().start()

    def start_f(u):
        if live(u):
            a = stage_a(u)
            a[0]().wait_recv()
            a[1]().wait_recv()
            for c in stage_f(u):
                c().start()
            if u % 2 == 0:
                t = stage_t(span(u)[0])
                t[0]().wait_recv()
                t[2]().start()

    def relay(u):
        if live(u):
            start_f(u)
            p = order.index(u)
            for w in range(ahead(p - 1), ahead(p)):
                start_a(order[w])

    def start_g(u):
        if live(u):
            a, f = stage_a(u), stage_f(u)
            f[0]().wait_recv()
            f[1]().wait_recv()
            g = stage_g(u)
            for c in g:
                c().start()
            if u % 2 == 0:
                for c in stage_t(span(u)[0])[1:]:
                    c().wait_recv()
            for c in (a[2], f[2], f[3], g[0], g[1]):
                c().wait_recv()

    def drain(u):
        if live(u):
            if u % 2 == 0:
                for c in stage_t(span(u)[0]):
                    c().wait_send()
            for c in (*stage_a(u), *stage_f(u), *stage_g(u)):
                c().wait_send()

    for w in range(ahead(-1)):
        start_a(order[w])
    t_copy = pltpu.make_async_copy(t_ref, tg.at[:, q_own], z_sem.at[1])
    t_copy.start()
    z_copy = pltpu.make_async_copy(z_ref, x_ref, z_sem.at[0])
    z_copy.start()
    relay(0)
    t_copy.wait()
    z_copy.wait()

    lane = lax.broadcasted_iota(jnp.int32, (64, LANES), 1)
    row_h = (lax.broadcasted_iota(jnp.int32, (LANES, LANES), 0) // 64) % 2
    col_h = (lax.broadcasted_iota(jnp.int32, (LANES, LANES), 1) // 64) % 2
    same_half = jnp.where(row_h == col_h, 1.0, 0.0).astype(F32)
    next_half = jnp.where(row_h < col_h, 1.0, 0.0).astype(F32)
    one = functools.partial(lax.dot_general, dimension_numbers=NN, preferred_element_type=F32)

    def block_step(i, carry):
        s = blocks - 1 - i
        n = i + 1
        n_first = (n + 1) // 2

        def row_of(t):
            return pl.multiple_of((s + t) * STRIP, STRIP)

        def x_rows(t):
            r = row_of(t)
            return (pl.ds(pl.multiple_of(y * half_rows + r, STRIP), STRIP),
                    pl.ds(pl.multiple_of((1 - y) * half_rows + r, STRIP), STRIP))

        def keep(t):
            return pl.ds(pl.multiple_of(t * 2 * STRIP, 2 * STRIP), 2 * STRIP)

        def put(src, slot, dy, q, k):
            return pltpu.make_async_copy(
                src, vbuf.at[slot, pl.ds(dy * STRIP, STRIP), pl.ds(pl.multiple_of(q * LANES, LANES), LANES)],
                load_sem.at[slot, dy, k])

        def load(t, slot):
            r = pl.ds(row_of(t), STRIP)
            put(v_ref.at[r, pl.ds(pl.multiple_of(s * LANES, LANES), LANES)], slot, 0, q_own, 0).start()
            for k, q in ((1, q_x), (2, q_c), (3, q_xc)):
                put(vg.at[s, y, q, r], slot, 0, q, k).start()
            for k, q in ((0, q_own), (1, q_x), (2, q_c), (3, q_xc)):
                put(vg.at[s, 1 - y, q, r], slot, 1, q, k).start()

        def load_wait(slot):
            for dy in (0, 1):
                for k, q in ((0, q_own), (1, q_x), (2, q_c), (3, q_xc)):
                    put(vg.at[0, 0, 0, pl.ds(0, STRIP)], slot, dy, q, k).wait()

        def take_in(lo, hi):
            @pl.when(lo < hi)
            def _():
                load(lo, lax.rem(lo, 2))

            def body(t, c):
                slot = lax.rem(t, 2)

                @pl.when(t + 1 < hi)
                def _():
                    load(t + 1, 1 - slot)

                load_wait(slot)
                v1, v2, v3 = split3(vbuf[slot])
                v1s[keep(t), :] = v1
                v2s[keep(t), :] = v2
                v3s[keep(t), :] = v3
                mine = pl.ds(pl.multiple_of((t * 2 + core) * STRIP, STRIP), STRIP)
                v1, v2, v3 = v1s[mine, :], v2s[mine, :], v3s[mine, :]
                v1t = v1.T
                v2t = v2.T
                gram[...] += one(jnp.concatenate([v2t, v1t], axis=1), jnp.concatenate([v2, v1], axis=0))
                gram_q[...] += one(jnp.concatenate([v1t, v1t], axis=1), jnp.concatenate([v3, v2], axis=0))
                return c

            lax.fori_loop(lo, hi, body, 0)

        def project(lo, hi):
            def body(t, c):
                own, other = x_rows(t)
                xs = split3(jnp.concatenate([x_ref[own, :].T, x_ref[other, :].T], axis=1))
                wt[...] += dot6(xs, (v1s[keep(t), :], v2s[keep(t), :], v3s[keep(t), :]), NN)
                return c

            lax.fori_loop(lo, hi, body, 0)

        wt[...] = jnp.zeros_like(wt)
        gram[...] = jnp.zeros_like(gram)
        gram_q[...] = jnp.zeros_like(gram_q)

        for k in range(blocks):
            @pl.when(i == k)
            def _():
                start_g(2 * k)

        take_in(0, n_first)
        project(0, n_first)

        for k in range(blocks):
            @pl.when(i == k)
            def _():
                start_g(2 * k + 1)
                relay(2 * k + 2)

        take_in(n_first, n)
        gq = gram_q[...]
        gram[...] += gq + gq.T
        slot = lax.rem(i, 2)
        g_copy = pltpu.make_async_remote_copy(
            src_ref=gram, dst_ref=g_in.at[slot], send_sem=gsend_sem.at[slot], recv_sem=grecv_sem.at[slot],
            device_id=dev_c, device_id_type=MESH_ID)
        g_copy.start()
        project(n_first, n)
        g_copy.wait()
        g = gram[...] + g_in[slot]

        tq = []
        for q in range(4):
            tt = tg[s, q]
            tq.append(jnp.concatenate([jnp.where(lane < 64, tt, 0.0), jnp.where(lane >= 64, tt, 0.0)], axis=0))

        def gq_blk(a, b):
            return g[a * LANES:(a + 1) * LANES, b * LANES:(b + 1) * LANES]

        def merge(ta, gab, tb):
            return -exact(exact(ta, gab, NN), tb, NN)

        zero = jnp.zeros((LANES, LANES), F32)
        t01 = merge(tq[0], gq_blk(0, 1) * same_half, tq[1])
        t23 = merge(tq[2], gq_blk(2, 3) * same_half, tq[3])
        ta = jnp.concatenate([jnp.concatenate([tq[0], t01], axis=1), jnp.concatenate([zero, tq[1]], axis=1)], axis=0)
        tb = jnp.concatenate([jnp.concatenate([tq[2], t23], axis=1), jnp.concatenate([zero, tq[3]], axis=1)], axis=0)
        gab = jnp.concatenate([jnp.concatenate([gq_blk(a, b) * same_half for b in (2, 3)], axis=1) for a in (0, 1)], axis=0)
        tab = merge(ta, gab, tb)
        zero2 = jnp.zeros((2 * LANES, 2 * LANES), F32)
        tfull = jnp.concatenate([jnp.concatenate([ta, tab], axis=1), jnp.concatenate([zero2, tb], axis=1)], axis=0)
        g3 = jnp.concatenate([jnp.concatenate([gq_blk(a, b) * next_half for b in range(4)], axis=1) for a in range(4)], axis=0)

        y1t = exact(wt[...], tfull, NT)
        yt = y1t - exact(exact(y1t, g3, NT), tfull, NT)
        ys = split3(yt.T)

        for k in range(blocks):
            @pl.when(i == k)
            def _():
                relay(2 * k + 3)

        def pass_two(t, c):
            own, other = x_rows(t)
            u = dot6((v1s[keep(t), :], v2s[keep(t), :], v3s[keep(t), :]), ys, NN)
            x_ref[own, :] = x_ref[own, :] - u[:STRIP]
            x_ref[other, :] = x_ref[other, :] - u[STRIP:]
            return c

        lax.fori_loop(0, n, pass_two, 0)
        return carry

    lax.fori_loop(0, blocks, block_step, 0)
    out = pltpu.make_async_copy(x_ref, x_out, z_sem.at[0])
    out.start()
    for u in range(units):
        drain(u)
    out.wait()


def solution(mesh):
    def local_apply(v_loc, t_loc, z_loc):
        n, k = z_loc.shape
        blocks = v_loc.shape[1] // LANES
        half_rows = v_loc.shape[0]
        wide = 4 * LANES
        t_pack = t_loc.reshape(blocks, 2, 64, 64).transpose(0, 2, 1, 3).reshape(blocks, 64, LANES)
        hbm = pl.BlockSpec(memory_space=pl.ANY)
        x_new, _ = pl.pallas_call(
            functools.partial(kernel, blocks),
            out_shape=(jax.ShapeDtypeStruct((n, k), F32),
                       jax.ShapeDtypeStruct((blocks, 2, 4, half_rows, LANES), F32)),
            in_specs=[hbm, pl.BlockSpec(memory_space=pltpu.VMEM), hbm],
            out_specs=(hbm, hbm),
            scratch_shapes=[
                pltpu.VMEM((n, k), F32),
                pltpu.VMEM((blocks, 4, 64, LANES), F32),
                pltpu.VMEM((2, 2 * STRIP, wide), F32),
                pltpu.VMEM((n, wide), BF16),
                pltpu.VMEM((n, wide), BF16),
                pltpu.VMEM((n, wide), BF16),
                pltpu.VMEM((k, wide), F32),
                pltpu.VMEM((wide, wide), F32),
                pltpu.VMEM((wide, wide), F32),
                pltpu.VMEM((2, wide, wide), F32),
                pltpu.SemaphoreType.DMA((2 * blocks, 9)),
                pltpu.SemaphoreType.DMA((2 * blocks, 9)),
                pltpu.SemaphoreType.DMA((blocks, 3)),
                pltpu.SemaphoreType.DMA((blocks, 3)),
                pltpu.SemaphoreType.DMA((2,)),
                pltpu.SemaphoreType.DMA((2,)),
                pltpu.SemaphoreType.DMA((2, 2, 4)),
                pltpu.SemaphoreType.DMA((2,)),
            ],
            compiler_params=pltpu.CompilerParams(has_side_effects=True, vmem_limit_bytes=64000 * 1024),
        )(v_loc, t_pack, z_loc)
        return x_new

    return jax.shard_map(
        local_apply,
        mesh=mesh,
        in_specs=(P("row", "col"), P("col", None, None), P(None, ("row", "col"))),
        out_specs=P(None, ("row", "col")),
        check_vma=False,
    )
```
